128 devices in a mesh: tp: 16 (over z, y), dp: 8 (over x, core).
Axes of the slice: x: 4, y: 4, z: 4, core: 2. Of those that a mesh axis runs over, the one named last changes fastest.
Arguments:
- hidden: bfloat16 [16, 512, 1536], P('dp')
- gamma: float32 [1536], replicated
- w_head: bfloat16 [1536, 151936], P(None, 'tp')
- labels: int32 [16, 512], P('dp')
- mask: int32 [16, 512], P('dp')
Outputs:
- output 1: float32 [], replicated
- output 2: bfloat16 [16, 512, 1536], P('dp')
- output 3: float32 [1536, 151936], P(None, 'tp')
- output 4: float32 [1536], replicated
All inputs are finite; a program needn't handle non-finite values.
Results may differ from the reference program's by a relative error of at most 0.001.
Values sent between devices are 32-bit elements.
A program may use at most 1 GiB of HBM per device.

```python
import math
import jax
import jax.numpy as jnp
from jax import lax

DP_RANKS = 8
BATCH_DEV = 2
SEQ = 512
DMODEL = 1536
VOCAB = 151936

BATCH = DP_RANKS * BATCH_DEV
EPS = 1e-5


def draw_labels(label_key):
    label_ids = jax.random.randint(label_key, (BATCH, SEQ), 0, VOCAB)
    return label_ids.at[0, 0].set(0).at[0, 1].set(VOCAB - 1)


def draw_mask(mask_key):
    dead_key, length_key = jax.random.split(mask_key)
    dead_count = jax.random.randint(dead_key, (DP_RANKS,), 0, BATCH_DEV // 2 + 1)
    dead_count = dead_count.at[0].set(BATCH_DEV // 2).at[1].set(0)
    seq_length = jax.random.randint(length_key, (BATCH,), SEQ // 2, SEQ + 1)
    seq_length = seq_length.at[0].set(SEQ // 2).at[BATCH_DEV].set(SEQ)
    seq_slot = jnp.arange(BATCH_DEV)[None, :]
    is_alive = (seq_slot < BATCH_DEV - dead_count[:, None]).reshape(BATCH)
    seq_length = jnp.where(is_alive, seq_length, 0)
    return (jnp.arange(SEQ)[None, :] < seq_length[:, None]).astype(jnp.int32)


def setup_inputs(seed: int = 0) -> dict:
    root_key = jax.random.key(seed)
    key_w, key_h, key_g, key_l, key_m = jax.random.split(root_key, 5)
    w_f32 = jax.random.normal(key_w, (DMODEL, VOCAB), jnp.float32) * DMODEL ** -0.5
    labels = draw_labels(key_l)
    mask = draw_mask(key_m)
    margin = math.log(VOCAB) - 1.0
    lift = margin * math.sqrt(DMODEL / (DMODEL - margin * margin))
    label_cols = jnp.take(w_f32, labels.reshape(BATCH * SEQ), axis=1).T.reshape(BATCH, SEQ, DMODEL)
    noise = jax.random.normal(key_h, (BATCH, SEQ, DMODEL), jnp.float32)
    hidden = (noise + lift * label_cols).astype(jnp.bfloat16)
    gamma = 1.0 + 0.2 * jax.random.normal(key_g, (DMODEL,), jnp.float32)
    return {"hidden": hidden, "gamma": gamma, "w_head": w_f32.astype(jnp.bfloat16), "labels": labels, "mask": mask}


def reference(hidden, gamma, w_head, labels, mask):
    tok_count = jnp.sum(mask).astype(jnp.float32)
    vocab_ids = jnp.arange(VOCAB)

    def seq_step(carry, seq_inputs):
        grad_w, grad_gamma, loss_sum = carry
        seq_hidden, seq_labels, seq_mask = seq_inputs
        tok_rows = seq_hidden.astype(jnp.float32)
        inv_rms = lax.rsqrt(jnp.mean(tok_rows * tok_rows, axis=-1, keepdims=True) + EPS)
        normed = tok_rows * inv_rms
        unit_rows = (normed * gamma).astype(jnp.bfloat16)
        logits = jnp.dot(unit_rows, w_head, preferred_element_type=jnp.float32)
        log_norm = jax.nn.logsumexp(logits, axis=-1)
        is_label = seq_labels[:, None] == vocab_ids[None, :]
        label_logit = jnp.sum(jnp.where(is_label, logits, 0.0), axis=-1)
        weight = seq_mask.astype(jnp.float32) / tok_count
        loss_sum = loss_sum + jnp.sum(weight * (log_norm - label_logit))
        soft_probs = jnp.exp(logits - log_norm[:, None])
        grad_logits = (jnp.where(is_label, soft_probs - 1.0, soft_probs) * weight[:, None]).astype(jnp.bfloat16)
        grad_w = grad_w + jnp.dot(unit_rows.T, grad_logits, preferred_element_type=jnp.float32)
        grad_unit = lax.dot_general(grad_logits, w_head, (((1,), (1,)), ((), ())), preferred_element_type=jnp.float32)
        grad_gamma = grad_gamma + jnp.sum(grad_unit * normed, axis=0)
        grad_normed = grad_unit * gamma
        grad_rows = inv_rms * (grad_normed - normed * jnp.mean(grad_normed * normed, axis=-1, keepdims=True))
        return (grad_w, grad_gamma, loss_sum), grad_rows.astype(jnp.bfloat16)

    start_carry = (jnp.zeros((DMODEL, VOCAB), jnp.float32), jnp.zeros((DMODEL,), jnp.float32), jnp.zeros((), jnp.float32))
    (grad_w, grad_gamma, total_loss), grad_hidden = lax.scan(seq_step, start_carry, (hidden, labels, mask))
    return total_loss, grad_hidden, grad_w, grad_gamma
```

```python
import functools

import jax
import jax.numpy as jnp
from jax import lax
from jax.experimental import pallas as pl
from jax.experimental.pallas import tpu as pltpu
from jax.sharding import Mesh, PartitionSpec as P

EPS = 1e-5
F32=jnp.float32; BF16=jnp.bfloat16
ANY = pl.BlockSpec(memory_space=pl.ANY)
SMEM = pl.BlockSpec(memory_space=pltpu.SMEM)
VMEM = pl.BlockSpec(memory_space=pltpu.VMEM)
D=1536; VL=9496; GROUP=16; CHUNK=512; PER=CHUNK//GROUP
BIG=1e30
def params(mib, **kw):
    return pltpu.CompilerParams(vmem_limit_bytes=mib * 1024 * 1024, **kw)
def cost(flops, nbytes):
    return pl.CostEstimate(flops=int(flops), bytes_accessed=int(nbytes), transcendentals=0)

def gw_kernel(segs, scal, tbl, winv_ref, sl_ref, u_hbm, w_hbm, out_in, out_ref, *rest):
    del out_in
    n = len(segs)
    sends, (ubuf, wbuf, acc, u_sem, w_sem, o_sem) = rest[:n], rest[n:]
    steps = scal[0]
    offs = [sum(segs[:k]) for k in range(n)]
    rows = [pl.multiple_of(scal[1 + k], 8) for k in range(n)]

    def fetch(i, slot):
        for g in range(PER):
            src = pl.multiple_of(tbl[i * PER + g], GROUP)
            pltpu.make_async_copy(u_hbm.at[pl.ds(src, GROUP), :], ubuf.at[slot, pl.ds(g * GROUP, GROUP), :], u_sem.at[slot]).start()

    cps = []
    for k, size in enumerate(segs):
        cps.append(pltpu.make_async_copy(w_hbm.at[pl.ds(rows[k], size), :], wbuf.at[pl.ds(offs[k], size), :], w_sem.at[k]))
    for cp in cps:
        cp.start()
    fetch(0, 0)
    acc[...] = jnp.zeros_like(acc)
    for cp in cps:
        cp.wait()
    winv = winv_ref[0]

    def body(i, _):
        slot = lax.rem(i, 2)
        pltpu.make_async_copy(u_hbm.at[pl.ds(0, CHUNK), :], ubuf.at[slot], u_sem.at[slot]).wait()
        fetch(jnp.minimum(i + 1, steps - 1), 1 - slot)
        u = ubuf[slot].astype(BF16)
        z = lax.dot_general(wbuf[...], u, (((1,), (1,)), ((), ())), preferred_element_type=F32)
        shift = sl_ref[0, pl.ds(i, 1), :]
        lab = sl_ref[1, pl.ds(i, 1), :]
        gs = []
        for k, size in enumerate(segs):
            ids = lax.broadcasted_iota(jnp.int32, (size, CHUNK), 0).astype(F32)
            rel = lab - rows[k].astype(F32)
            gs.append((jnp.exp(z[offs[k]:offs[k] + size] - shift) - jnp.where(ids == rel, winv, 0.0)).astype(BF16))
        g = jnp.concatenate(gs, axis=0) if n > 1 else gs[0]
        acc[...] += jnp.dot(g, u, preferred_element_type=F32)
        return 0

    lax.fori_loop(0, steps, body, 0)
    pltpu.make_async_copy(u_hbm.at[pl.ds(0, CHUNK), :], ubuf.at[0], u_sem.at[lax.rem(steps, 2)]).wait()
    cps = []
    for k, size in enumerate(segs):
        src = acc.at[pl.ds(offs[k], size), :]
        cps.append(pltpu.make_async_copy(src, sends[k], o_sem.at[2 * k]))
        cps.append(pltpu.make_async_copy(src, out_ref.at[pl.ds(rows[k], size), :], o_sem.at[2 * k + 1]))
    for cp in cps:
        cp.start()
    for cp in cps:
        cp.wait()

def gw_call(segs, scal, tbl, winv, sl, u, w, out):
    n = len(segs)
    width = sum(segs)
    dma = pltpu.SemaphoreType.DMA
    res = pl.pallas_call(
        functools.partial(gw_kernel, segs),
        in_specs=[SMEM, SMEM, SMEM, VMEM] + [ANY] * 3,
        out_specs=[ANY] * (n + 1),
        out_shape=[jax.ShapeDtypeStruct((VL, D), F32)] + [jax.ShapeDtypeStruct((s, D), F32) for s in segs],
        scratch_shapes=[
            pltpu.VMEM((2, CHUNK, D), F32),
            pltpu.VMEM((width, D), BF16), pltpu.VMEM((width, D), F32),
            dma((2,)), dma((n,)), dma((2 * n,)),
        ],
        input_output_aliases={6: 0},
        compiler_params=params(48),
        cost_estimate=cost(2 * 2 * 5000 * D * width, 40e6),
        name="grad_w_" + str(width),
    )(scal, tbl, winv, sl, u, w, out)
    return res[0], res[1:]

MESH = pl.DeviceIdType.MESH
VB=512; NFULL=VL//VB; TAIL=VL-NFULL*VB
ROWS=1024


def own_kernel(uf, ub_ref, w_hbm, meta_ref, u_out, du_out, sl_ref, meta_out, misc_ref,
               z_ref, wbuf, du, m_ref, s_ref, l_ref, st_buf, st_mine, lz_buf,
               ssem, rsem, s_send, s_recv, m_send, m_recv, l_send, l_recv, w_sem, c_sem):
    zi, yi, xi, ci = (lax.axis_index(n) for n in ("z", "y", "x", "c"))
    tp = zi * 4 + yi
    rank = xi * 2 + ci
    up = lambda i: lax.rem(i + 1, 4)
    dn = lambda i: lax.rem(i + 3, 4)
    op = lambda i: lax.rem(i + 2, 4)
    xp, xm, x2 = up(xi), dn(xi), op(xi)
    yp, ym, y2 = up(yi), dn(yi), op(yi)
    zp, zm, z2 = up(zi), dn(zi), op(zi)
    plane = [lax.rem(tp + k, 16) for k in range(1, 16)]
    line = [lax.rem(rank + k, 8) for k in range(1, 8)]
    pid = lambda q: {"z": q // 4, "y": lax.rem(q, 4)}
    lid = lambda q: {"x": q // 2, "c": lax.rem(q, 2)}

    def remote(src, dst, ssem_, rsem_, dev):
        return pltpu.make_async_remote_copy(src_ref=src, dst_ref=dst, send_sem=ssem_, recv_sem=rsem_, device_id=dev, device_id_type=MESH)

    lo, hi, al = pl.ds(0, 32), pl.ds(32, 32), pl.ds(0, 4)

    def regions(c):
        rm, rp, r2 = 2 * xm + c, 2 * xp + c, 2 * x2 + c
        a0 = lambda z, y: u_out.at[rm, z, y, lo]
        b0 = lambda z, y: u_out.at[r2, z, y, lo]
        a1 = lambda z, y: u_out.at[rp, z, y, lo]
        b1 = lambda z, y: u_out.at[r2, z, y, hi]
        return dict(
            a0=a0, b0=b0, a1=a1, b1=b1,
            a0row=lambda z: u_out.at[rm, z, al, lo], b0row=lambda z: u_out.at[r2, z, al, lo],
            a1col=lambda y: u_out.at[rp, al, y, lo], b1col=lambda y: u_out.at[r2, al, y, hi],
            xdm=u_out.at[rm, al, al, hi], xdp=u_out.at[rp, al, al, hi], x2=u_out.at[r2, zi, yi],
        )

    R = regions(ci)
    X_P, X_M, X_2 = {"x": xp}, {"x": xm}, {"x": x2}
    Y_P, Y_M, Z_P, Z_M, PAL = {"y": yp}, {"y": ym}, {"z": zp}, {"z": zm}, {"c": 1 - ci}
    msgs = {}

    def add(k, src, dev, arrives, dst=None):
        msgs[k] = (src, src if dst is None else dst, dev, arrives)

    mine = uf.at[zi, yi]
    add(0, uf.at[zi, yi, lo], X_P, R["a0"](zi, yi), u_out.at[rank, zi, yi, lo])
    add(1, uf.at[zi, yi, lo], X_M, R["a1"](zi, yi), u_out.at[rank, zi, yi, lo])
    add(2, mine, X_2, R["x2"], u_out.at[rank, zi, yi])
    add(3, uf.at[al, al, hi], X_P, R["xdm"], u_out.at[rank, al, al, hi])
    add(4, uf.at[al, al, hi], X_M, R["xdp"], u_out.at[rank, al, al, hi])
    add(5, R["a0"](zi, yi), Y_P, R["a0"](zi, ym))
    add(6, R["a0"](zi, yi), Y_M, R["a0"](zi, yp))
    add(7, R["b0"](zi, yi), Y_P, R["b0"](zi, ym))
    add(8, R["b0"](zi, yi), Y_M, R["b0"](zi, yp))
    add(9, R["a0"](zi, ym), Y_P, R["a0"](zi, y2))
    add(10, R["b0"](zi, yp), Y_M, R["b0"](zi, y2))
    add(11, R["a0row"](zi), Z_P, R["a0row"](zm))
    add(12, R["a0row"](zi), Z_M, R["a0row"](zp))
    add(13, R["b0row"](zi), Z_P, R["b0row"](zm))
    add(14, R["b0row"](zi), Z_M, R["b0row"](zp))
    add(15, R["a0row"](zm), Z_P, R["a0row"](z2))
    add(16, R["b0row"](zp), Z_M, R["b0row"](z2))
    add(17, R["a1"](zi, yi), Z_P, R["a1"](zm, yi))
    add(18, R["a1"](zi, yi), Z_M, R["a1"](zp, yi))
    add(19, R["b1"](zi, yi), Z_P, R["b1"](zm, yi))
    add(20, R["b1"](zi, yi), Z_M, R["b1"](zp, yi))
    add(21, R["a1"](zm, yi), Z_P, R["a1"](z2, yi))
    add(22, R["b1"](zp, yi), Z_M, R["b1"](z2, yi))
    add(23, R["a1col"](yi), Y_P, R["a1col"](ym))
    add(24, R["a1col"](yi), Y_M, R["a1col"](yp))
    add(25, R["b1col"](yi), Y_P, R["b1col"](ym))
    add(26, R["b1col"](yi), Y_M, R["b1col"](yp))
    add(27, R["a1col"](ym), Y_P, R["a1col"](y2))
    add(28, R["b1col"](yp), Y_M, R["b1col"](y2))
    Q = regions(1 - ci)
    add(29, uf, PAL, u_out.at[2 * xi + 1 - ci], u_out.at[rank])
    add(30, R["xdm"], PAL, Q["xdm"])
    add(31, R["xdp"], PAL, Q["xdp"])
    for k, (n, i) in enumerate([("a0row", zi), ("b0row", zi), ("a0row", zm), ("a0row", zp), ("a0row", z2), ("b0row", zm), ("b0row", zp), ("b0row", z2),
                                ("a1col", yi), ("b1col", yi), ("a1col", ym), ("a1col", yp), ("a1col", y2), ("b1col", ym), ("b1col", yp), ("b1col", y2)]):
        add(32 + k, R[n](i), PAL, Q[n](i))

    def send(*ks):
        for k in ks:
            src, dst, dev, _ = msgs[k]
            remote(src, dst, ssem.at[k], rsem.at[k], dev).start()

    def got(*ks):
        for k in ks:
            _, _, dev, reg = msgs[k]
            remote(reg, reg, ssem.at[k], rsem.at[k], dev).wait_recv()

    def sent(*ks):
        for k in ks:
            src, dst, dev, _ = msgs[k]
            remote(src, dst, ssem.at[k], rsem.at[k], dev).wait_send()

    bar = pltpu.get_barrier_semaphore()
    for q in plane:
        pl.semaphore_signal(bar, inc=1, device_id=pid(q), device_id_type=MESH)
    for q in line:
        pl.semaphore_signal(bar, inc=1, device_id=lid(q), device_id_type=MESH)
    pl.semaphore_wait(bar, 22)

    def w_copy(j, slot, size=VB):
        return pltpu.make_async_copy(w_hbm.at[pl.ds(pl.multiple_of(j * VB, VB), size), :], wbuf.at[slot, pl.ds(0, size)], w_sem.at[slot])

    w_copy(0, 0).start()
    line_msgs = []
    for k, q in enumerate(line):
        cp = remote(meta_ref, meta_out.at[rank], m_send.at[k], m_recv.at[rank], lid(q))
        cp.start()
        line_msgs.append(cp)
    send(0, 1, 2, 3, 4, 29)
    stage = [(uf.at[t // 4, t % 4], du.at[pl.ds(64 * t, 64)], u_out.at[rank, t // 4, t % 4]) for t in range(16)]
    for a, b, _ in stage:
        pltpu.make_async_copy(a, b, c_sem.at[0]).start()
    meta_out[rank] = meta_ref[...]
    m_ref[...] = jnp.full_like(m_ref, -BIG)
    s_ref[...] = jnp.zeros_like(s_ref)
    l_ref[...] = jnp.zeros_like(l_ref)

    def as_row(v):
        return jnp.concatenate([v[i:i + 1, :] for i in range(8)], axis=1)

    lab = as_row((meta_ref[0] - tp * VL).astype(F32))

    def stats(j, slot, size):
        z = lax.dot_general(wbuf[slot, :size], ub_ref[...], (((1,), (1,)), ((), ())), preferred_element_type=F32)
        z_ref[pl.ds(pl.multiple_of(j * VB, VB), size), :] = z
        zz = z.reshape(size // 8, 8, ROWS)
        ids = lax.broadcasted_iota(jnp.int32, (size, ROWS), 0).astype(F32)
        rel = lab - (j * VB) * 1.0
        m_old = m_ref[...]
        m_new = jnp.maximum(m_old, jnp.max(zz, axis=0))
        s_ref[...] = s_ref[...] * jnp.exp(m_old - m_new) + jnp.sum(jnp.exp(zz - m_new[None]), axis=0)
        l_ref[...] += jnp.sum(jnp.where(ids == rel, z, 0.0).reshape(size // 8, 8, ROWS), axis=0)
        m_ref[...] = m_new

    def at(j, k, fn):
        @pl.when(j == k)
        def _():
            fn()

    def copy_out():
        for a, b, _ in stage:
            pltpu.make_async_copy(a, b, c_sem.at[0]).wait()
        for _, b, c in stage:
            pltpu.make_async_copy(b, c, c_sem.at[1]).start()

    def first_a():
        got(0, 1)
        send(5, 6, 17, 18)

    def first_b():
        got(2)
        send(7, 8, 19, 20)

    def hop_a():
        got(5, 17)
        send(9, 21)

    def hop_b():
        got(8, 20)
        send(10, 22)

    def stream(j):
        slot = lax.rem(j, 2)
        w_copy(j, slot).wait()

        @pl.when(j < NFULL - 1)
        def _():
            w_copy(j + 1, 1 - slot).start()

        @pl.when(j == NFULL - 1)
        def _():
            w_copy(NFULL, 1 - slot, TAIL).start()

        return slot

    def stats_step(j, _):
        slot = stream(j)
        stats(j, slot, VB)
        at(j, 2, copy_out)
        at(j, 4, first_a)
        at(j, 8, hop_a)
        at(j, 9, first_b)
        at(j, 13, hop_b)
        return 0

    lax.fori_loop(0, NFULL, stats_step, 0)
    w_copy(NFULL, NFULL % 2, TAIL).wait()
    stats(NFULL, NFULL % 2, TAIL)
    w_copy(0, 0).start()
    for _, b, c in stage:
        pltpu.make_async_copy(b, c, c_sem.at[1]).wait()

    m8 = m_ref[...]
    top = jnp.max(m8, axis=0, keepdims=True)
    tot = jnp.sum(s_ref[...] * jnp.exp(m8 - top), axis=0, keepdims=True)
    hit = jnp.sum(l_ref[...], axis=0, keepdims=True)

    def as_tile(v):
        return jnp.concatenate([v[:, 128 * i:128 * i + 128] for i in range(8)], axis=0)

    for k, v in enumerate((top, tot, hit)):
        st_mine[k] = as_tile(v)
        st_buf[tp, k] = as_tile(v)
    plane_msgs = []
    for k, q in enumerate(plane):
        cp = remote(st_mine, st_buf.at[tp], s_send.at[k], s_recv.at[tp], pid(q))
        cp.start()
        plane_msgs.append(cp)
    got(6, 9)
    send(11, 12, 32)
    got(18, 21)
    send(23, 24, 40)
    got(7, 10)
    send(13, 14, 33)
    got(19, 22)
    send(25, 26, 41)
    for k, q in enumerate(line):
        remote(meta_ref, meta_out.at[q], m_send.at[k], m_recv.at[q], lid(q)).wait_recv()
    count = jnp.zeros((8, 128), F32)
    for r in range(8):
        count += meta_out[r, 1].astype(F32)
    count = jnp.broadcast_to(jnp.sum(jnp.sum(count, axis=1, keepdims=True), axis=0, keepdims=True), (8, 128))
    log_n = jnp.log(count)
    for k, q in enumerate(plane):
        remote(st_mine, st_buf.at[q], s_send.at[k], s_recv.at[q], pid(q)).wait_recv()
    top = st_buf[0, 0]
    for q in range(1, 16):
        top = jnp.maximum(top, st_buf[q, 0])
    total = jnp.zeros_like(top)
    label = jnp.zeros_like(top)
    for q in range(16):
        total += st_buf[q, 1] * jnp.exp(st_buf[q, 0] - top)
        label += st_buf[q, 2]
    lse = top + jnp.log(total)
    lz_buf[rank, 0] = lse
    lz_buf[rank, 1] = label
    on = meta_ref[1] > 0
    shift = as_row(jnp.where(on, lse + log_n, BIG))
    lab_on = as_row(jnp.where(on, (meta_ref[0] - tp * VL).astype(F32), -BIG))
    winv = as_row(1.0 / count)
    for k, q in enumerate(line):
        cp = remote(lz_buf.at[rank], lz_buf.at[rank], l_send.at[k], l_recv.at[rank], lid(q))
        cp.start()
        line_msgs.append(cp)

    du[...] = jnp.zeros_like(du)

    def grad(j, slot, size):
        z = z_ref[pl.ds(pl.multiple_of(j * VB, VB), size), :]
        ids = lax.broadcasted_iota(jnp.int32, (size, ROWS), 0).astype(F32)
        rel = lab_on - (j * VB) * 1.0
        g = (jnp.exp(z - shift) - jnp.where(ids == rel, winv, 0.0)).astype(BF16)
        du[...] += lax.dot_general(g, wbuf[slot, :size], (((0,), (0,)), ((), ())), preferred_element_type=F32)

    def arrive_a():
        got(11)
        send(15, 34)
        got(23)
        send(27, 42)
        got(12)
        send(35)
        got(24)
        send(43)

    def arrive_b():
        got(14)
        send(16, 38)
        got(26)
        send(28, 46)
        got(13)
        send(37)
        got(25)
        send(45)

    def arrive_x():
        got(3)
        send(30)
        got(4)
        send(31)

    def grad_step(j, _):
        slot = stream(j)
        grad(j, slot, VB)
        at(j, 5, arrive_a)
        at(j, 13, arrive_b)
        at(j, 16, arrive_x)
        return 0

    lax.fori_loop(0, NFULL, grad_step, 0)
    w_copy(NFULL, NFULL % 2, TAIL).wait()
    grad(NFULL, NFULL % 2, TAIL)
    out = pltpu.make_async_copy(du, du_out, c_sem.at[0])
    out.start()

    for k, q in enumerate(line):
        remote(lz_buf.at[q], lz_buf.at[q], l_send.at[k], l_recv.at[q], lid(q)).wait_recv()
    loss = jnp.zeros((8, 128), F32)
    for r in range(8):
        on = meta_out[r, 1] > 0
        lse = lz_buf[r, 0]
        loss += jnp.where(on, (lse - lz_buf[r, 1]) / count, 0.0)
        sl_ref[0, r] = jnp.where(on, lse + log_n, BIG)
        sl_ref[1, r] = jnp.where(on, (meta_out[r, 0] - tp * VL).astype(F32), -BIG)
    loss = jnp.sum(jnp.sum(loss, axis=1, keepdims=True), axis=0, keepdims=True)
    sub = lax.broadcasted_iota(jnp.int32, (8, 128), 0)
    misc_ref[...] = jnp.where(sub == 0, jnp.broadcast_to(loss, (8, 128)), 1.0 / count)
    got(15)
    send(36)
    got(27)
    send(44)
    got(16)
    send(39)
    got(28)
    send(47)
    for k in range(29, 48):
        got(k)
    for cp in line_msgs + plane_msgs:
        cp.wait_send()
    sent(*range(48))
    out.wait()


def own_call(uf, ub, wt, meta):
    dma = pltpu.SemaphoreType.DMA
    return pl.pallas_call(
        own_kernel,
        in_specs=[ANY, VMEM, ANY, VMEM],
        out_specs=[ANY, ANY, VMEM, VMEM, VMEM],
        out_shape=[
            jax.ShapeDtypeStruct((8, 4, 4, 64, D), F32),
            jax.ShapeDtypeStruct((ROWS, D), F32),
            jax.ShapeDtypeStruct((2, 8, 8, 128), F32),
            jax.ShapeDtypeStruct((8, 2, 8, 128), jnp.int32),
            jax.ShapeDtypeStruct((8, 128), F32),
        ],
        scratch_shapes=[
            pltpu.VMEM((VL, ROWS), F32), pltpu.VMEM((2, VB, D), BF16), pltpu.VMEM((ROWS, D), F32),
            pltpu.VMEM((8, ROWS), F32), pltpu.VMEM((8, ROWS), F32), pltpu.VMEM((8, ROWS), F32),
            pltpu.VMEM((16, 3, 8, 128), F32), pltpu.VMEM((3, 8, 128), F32), pltpu.VMEM((8, 2, 8, 128), F32),
            dma((48,)), dma((48,)), dma((15,)), dma((16,)), dma((7,)), dma((8,)), dma((7,)), dma((8,)), dma((2,)), dma((2,)),
        ],
        compiler_params=params(62, collective_id=0, has_side_effects=True),
        cost_estimate=cost(4 * ROWS * D * VL, 200e6),
        name="own_rank",
    )(uf, ub, wt, meta)

SEG = 384
S_ROWS = 1536


def place_kernel(nsrc, rows, depth, where, *refs):
    srcs, out_ref, (buf, in_sem, out_sem) = refs[:nsrc], refs[nsrc + 1], refs[nsrc + 2:]
    jobs = []
    for k in range(nsrc):
        n = srcs[k].shape[0]
        for r in range(0, n, rows):
            jobs.append((k, r, min(rows, n - r)))

    def load(q):
        k, r, size = jobs[q]
        return pltpu.make_async_copy(srcs[k].at[pl.ds(r, size), :], buf.at[q % depth, pl.ds(0, size), :], in_sem.at[q % depth])

    def store(q):
        k, r, size = jobs[q]
        dst = out_ref.at[pl.ds(pl.multiple_of(where[k], 8) + r, size), :]
        return pltpu.make_async_copy(buf.at[q % depth, pl.ds(0, size), :], dst, out_sem.at[q % depth])

    lead = depth // 2
    for q in range(len(jobs) + lead):
        if q < len(jobs):
            if q >= depth:
                store(q - depth).wait()
            load(q).start()
        if q >= lead:
            load(q - lead).wait()
            store(q - lead).start()
    for q in range(max(0, len(jobs) - depth), len(jobs)):
        store(q).wait()


def place_call(where, srcs, out):
    rows, depth, n = 384, 8, len(srcs)
    dma = pltpu.SemaphoreType.DMA
    return pl.pallas_call(
        functools.partial(place_kernel, n, rows, depth),
        in_specs=[SMEM] + [ANY] * (n + 1),
        out_specs=ANY,
        out_shape=jax.ShapeDtypeStruct((VL, D), F32),
        scratch_shapes=[pltpu.VMEM((depth, rows, D), F32), dma((depth,)), dma((depth,))],
        input_output_aliases={n + 1: 0},
        compiler_params=params(32),
        cost_estimate=cost(1e10, 80e6),
        name="place_" + str(n),
    )(where, *srcs, out)


def alloc_kernel(x_ref, o_ref):
    del x_ref, o_ref


def alloc_out(dep):
    return pl.pallas_call(
        alloc_kernel, in_specs=[ANY], out_specs=ANY, out_shape=jax.ShapeDtypeStruct((VL, D), F32), name="alloc",
    )(dep)


def local_step(hidden, gamma, w, labels, mask):
    num_seqs, seqlen, _ = hidden.shape
    tokens = num_seqs * seqlen
    zi, yi, xi, ci = (lax.axis_index(n) for n in ("z", "y", "x", "c"))
    swap = [(0, 1), (1, 0)]
    wt = w.T

    rows = hidden.reshape(tokens, D).astype(F32)
    inv = lax.rsqrt(jnp.mean(rows * rows, axis=-1, keepdims=True) + EPS)
    u = (rows * inv * gamma).astype(BF16)
    meta = jnp.stack([labels.reshape(8, 128), mask.reshape(8, 128)])
    u_all, du, sl, meta_all, misc = own_call(u.astype(F32).reshape(4, 4, 64, D), u, wt, meta)
    u_all = u_all.reshape(8192, D)
    loss = misc[0, 0]
    winv = misc[1, 0].reshape(1)

    seq_len = meta_all[:, 1].reshape(16, 512).sum(-1)
    groups = (seq_len + GROUP - 1) // GROUP
    pos = jnp.arange(512)
    ids = jnp.arange(16)
    before = jnp.sum(jnp.where(ids[None, :] < ids[:, None], groups[None, :], 0), axis=1)
    total = jnp.sum(groups)
    seq = jnp.sum(pos[:, None] >= (before + groups)[None, :], axis=1)
    start = jnp.sum(jnp.where(ids[None, :] == seq[:, None], before[None, :], 0), axis=1)
    live = pos < total
    grp = jnp.where(live, seq * 32 + pos - start, 0)
    tbl = (grp * GROUP).astype(jnp.int32)
    steps = ((total + PER - 1) // PER).astype(jnp.int32)
    dead = jnp.stack([jnp.full((GROUP,), BIG, F32), jnp.full((GROUP,), -BIG, F32)])[:, None, :]
    slc = jnp.where(live[None, :, None], jnp.take(sl.reshape(2, 512, GROUP), grp, axis=1), dead).reshape(2, 16, CHUNK)

    half = 4752
    base = ci * half
    other = (1 - ci) * half
    even = xi % 2 == 0
    s_off = jnp.where(even, S_ROWS, 0)
    r_off = jnp.where(even, 0, S_ROWS)
    left = [(i, (i + 3) % 4) for i in range(4)]
    right = [(i, (i + 1) % 4) for i in range(4)]
    out = alloc_out(misc)
    pieces, where, hop = [], [], []
    sc = lambda *v: jnp.stack([steps, *v]).astype(jnp.int32)
    for k in range(2):
        offs = [SEG * k, S_ROWS // 2 + SEG * k]
        out, (sl_, sr_) = gw_call((SEG, SEG), sc(*[base + s_off + o for o in offs]), tbl, winv, slc, u_all, wt, out)
        rl = lax.ppermute(sl_, "x", left)
        rr = lax.ppermute(sr_, "x", right)
        for arr, o in ((rl, offs[0]), (rr, offs[1])):
            pieces.append(arr)
            where.append(base + r_off + o)
            hop.append((arr, other + r_off + o))
        for arr, o in ((sl_, offs[0]), (sr_, offs[1])):
            pieces.append(lax.ppermute(arr, "c", swap))
            where.append(other + s_off + o)
    c_off = 2 * S_ROWS
    for o, size in ((c_off, 840), (c_off + 840, 840)):
        lim = VL - size
        out, (cc,) = gw_call((size,), sc(jnp.minimum(base + o, lim)), tbl, winv, slc, u_all, wt, out)
        pieces.append(lax.ppermute(cc, "c", swap))
        where.append(jnp.minimum(other + o, lim))
    for arr, o in hop:
        pieces.append(lax.ppermute(arr, "c", swap))
        where.append(o)
    grad_w = place_call(jnp.stack(where).astype(jnp.int32), pieces, out).T

    du = lax.psum(du, ("z", "y"))
    n = rows * inv
    v = du * gamma
    grad_rows = inv * (v - n * jnp.mean(v * n, axis=-1, keepdims=True))
    grad_hidden = grad_rows.astype(BF16).reshape(num_seqs, seqlen, D)
    gg = jnp.sum(du * n, axis=0, keepdims=True)
    parts = [gg] + [lax.ppermute(gg, "x", [(i, (i + k) % 4) for i in range(4)]) for k in range(1, 4)]
    stack = jnp.concatenate(parts, axis=0)
    order = (xi - jnp.arange(4)) % 4
    gg = sum(jnp.take(stack, order[i:i + 1], axis=0) for i in range(4))
    grad_gamma = (gg + lax.ppermute(gg, "c", swap)).reshape(D)
    return loss, grad_hidden, grad_w, grad_gamma


def solution(mesh):
    fine = Mesh(mesh.devices.reshape(4, 4, 4, 2), ("z", "y", "x", "c"))
    return jax.shard_map(
        local_step,
        mesh=fine,
        in_specs=(P(("x", "c"), None, None), P(), P(None, ("z", "y")), P(("x", "c"), None), P(("x", "c"), None)),
        out_specs=(P(), P(("x", "c"), None, None), P(None, ("z", "y")), P()),
        check_vma=False,
    )
```

```python
import functools

import jax
import jax.numpy as jnp
from jax import lax
from jax.experimental import pallas as pl
from jax.experimental.pallas import tpu as pltpu
from jax.sharding import Mesh, PartitionSpec as P


EPS = 1e-5
D = 1536
VL = 9496
GROUP = 16
CHUNK = 1024
PER = CHUNK // GROUP
STEP = 512
BIG = 1e30
LANE = 128
SLICE = 64
ALL_ROWS = 8192
F32 = jnp.float32
BF16 = jnp.bfloat16
ANY = pl.BlockSpec(memory_space=pl.ANY)
SMEM = pl.BlockSpec(memory_space=pltpu.SMEM)
VMEM = pl.BlockSpec(memory_space=pltpu.VMEM)
DMA = pltpu.SemaphoreType.DMA


def params(mib, **kw):
    return pltpu.CompilerParams(vmem_limit_bytes=int(mib * 1024 * 1024), **kw)


def cost(flops, nbytes):
    return pl.CostEstimate(flops=int(flops), bytes_accessed=int(nbytes), transcendentals=0)


TBL = 640


def fill_table(cnt, tbl):
    def seq(s, n):
        g = (cnt[s] + GROUP - 1) // GROUP

        def one(k, _):
            tbl[n + k] = s * 512 + k * GROUP
            return 0

        lax.fori_loop(0, g, one, 0)
        return n + g

    total = lax.fori_loop(0, 16, seq, 0)
    steps = (total + STEP // GROUP - 1) // (STEP // GROUP)

    def dead(k, _):
        tbl[k] = ALL_ROWS
        return 0

    lax.fori_loop(total, ((steps + 1) // 2) * PER, dead, 0)
    tbl[576] = steps


def gw_kernel(first, last, segs, lands, spots_of, *refs):
    n, m = len(segs), len(lands)
    refs = list(refs)
    cnt, misc_ref = refs.pop(0), refs.pop(0)
    if first:
        u_hbm, sa_hbm, w_hbm = refs[:3]
        out_ref, refs = refs[3], refs[4:]
        sends, (uc_ref, side_ref, tbl), refs = refs[:n], refs[n:n + 3], refs[n + 3:]
        land = []
        fbuf, sbuf, f_sem, s_sem = refs[:4]
        refs = refs[4:]
    else:
        side_ref, uc_ref, w_hbm = refs[:3]
        land, out_ref, refs = refs[3:3 + m], refs[4 + m], refs[5 + m:]
        sends, refs = refs[:n], refs[n:]
        tbl = cnt
    ubuf, wbuf, acc, pbuf, u_sem, w_sem, o_sem, p_sem = refs
    offs = [sum(segs[:k]) for k in range(n)]
    rows, spots = spots_of()
    rows, spots = [pl.multiple_of(v, 8) for v in rows], [pl.multiple_of(v, 8) for v in spots]
    poff = [sum(lands[:k]) for k in range(m)]

    cps = [pltpu.make_async_copy(w_hbm.at[pl.ds(rows[k], size), :], wbuf.at[pl.ds(offs[k], size), :], w_sem.at[k]) for k, size in enumerate(segs)]
    for cp in cps:
        cp.start()
    loads = [pltpu.make_async_copy(land[k], pbuf.at[pl.ds(poff[k], size), :], p_sem.at[k]) for k, size in enumerate(lands)]
    stores = [pltpu.make_async_copy(pbuf.at[pl.ds(poff[k], size), :], out_ref.at[pl.ds(spots[k], size), :], p_sem.at[k]) for k, size in enumerate(lands)]
    if first:
        fill_table(cnt, tbl)
    steps = tbl[576]
    whole = steps // 2
    chunks = (steps + 1) // 2

    def gather(i, slot):
        for g in range(PER):
            src = tbl[i * PER + g]
            to = pl.ds(g * GROUP, GROUP)
            srow = pl.multiple_of(src, GROUP)
            urow = pl.multiple_of(jnp.where(src == ALL_ROWS, 0, src), GROUP)
            pltpu.make_async_copy(u_hbm.at[pl.ds(urow, GROUP), :], fbuf.at[slot, to, :], f_sem.at[slot]).start()
            pltpu.make_async_copy(sa_hbm.at[pl.ds(srow, GROUP), :], sbuf.at[slot, to, :], s_sem.at[slot]).start()

    def chunk_copy(i, slot, back):
        to = pl.ds(pl.multiple_of(i * CHUNK, CHUNK), CHUNK)
        if back:
            return pltpu.make_async_copy(ubuf.at[slot], uc_ref.at[to, :], u_sem.at[slot])
        return pltpu.make_async_copy(uc_ref.at[to, :], ubuf.at[slot], u_sem.at[slot])

    def begin(i, slot):
        if first:
            gather(i, slot)
        else:
            chunk_copy(i, slot, False).start()

    def arrive(i, slot):
        if first:
            pltpu.make_async_copy(u_hbm.at[pl.ds(0, CHUNK), :], fbuf.at[slot], f_sem.at[slot]).wait()
            pltpu.make_async_copy(sa_hbm.at[pl.ds(0, CHUNK), :], sbuf.at[slot], s_sem.at[slot]).wait()

            @pl.when(i >= 2)
            def _():
                chunk_copy(i - 2, slot, True).wait()
        else:
            chunk_copy(i, slot, False).wait()

    def unpack(i, slot):
        ubuf[slot] = fbuf[slot].astype(BF16)
        for k in range(CHUNK // LANE):
            t = jnp.transpose(sbuf[slot, LANE * k:LANE * k + LANE])
            side_ref[i, 0:1, LANE * k:LANE * k + LANE] = t[0:1]
            side_ref[i, 1:2, LANE * k:LANE * k + LANE] = t[SLICE:65]
        chunk_copy(i, slot, True).start()

    begin(0, 0)
    acc[...] = jnp.zeros_like(acc)
    winv = misc_ref[1, 0]
    for cp in cps:
        cp.wait()

    def work(i, slot, size):
        u = ubuf[slot, :size]
        z = lax.dot_general(wbuf[...], u, (((1,), (1,)), ((), ())), preferred_element_type=F32)
        shift = side_ref[i, 0:1, :size]
        lab = side_ref[i, 1:2, :size]
        gs = []
        for k, rs in enumerate(segs):
            ids = lax.broadcasted_iota(jnp.int32, (rs, size), 0).astype(F32)
            rel = lab - rows[k].astype(F32)
            gs.append((jnp.exp(z[offs[k]:offs[k] + rs] - shift) - jnp.where(ids == rel, winv, 0.0)).astype(BF16))
        g = jnp.concatenate(gs, axis=0) if n > 1 else gs[0]
        acc[...] += jnp.dot(g, u, preferred_element_type=F32)

    def body(i, _):
        slot = lax.rem(i, 2)
        arrive(i, slot)
        begin(jnp.minimum(i + 1, chunks - 1), 1 - slot)
        for p in range(m):
            @pl.when(i == jnp.minimum(p, whole - 1))
            def _():
                loads[p].start()

            @pl.when(i == p + 1)
            def _():
                loads[p].wait()
                stores[p].start()
        if first:
            unpack(i, slot)
        work(i, slot, CHUNK)
        return 0

    lax.fori_loop(0, whole, body, 0)
    for p in range(m):
        @pl.when(p + 1 >= whole)
        def _():
            loads[p].wait()
            stores[p].start()
    tail = lax.rem(whole, 2)
    if first:
        pltpu.make_async_copy(u_hbm.at[pl.ds(0, CHUNK), :], fbuf.at[tail], f_sem.at[tail]).wait()
        pltpu.make_async_copy(sa_hbm.at[pl.ds(0, CHUNK), :], sbuf.at[tail], s_sem.at[tail]).wait()
        chunk_copy(0, tail, True).wait()
    else:
        chunk_copy(0, tail, False).wait()

    @pl.when(chunks > whole)
    def _():
        if first:
            unpack(whole, tail)
        work(whole, tail, STEP)
        if first:
            chunk_copy(0, tail, True).wait()

    if first:
        chunk_copy(0, 1 - tail, True).wait()
    cps = []
    for k, size in enumerate(segs):
        src = acc.at[pl.ds(offs[k], size), :]
        cps.append(pltpu.make_async_copy(src, sends[k], o_sem.at[2 * k]))
        if last:
            cps.append(pltpu.make_async_copy(src, out_ref.at[pl.ds(rows[k], size), :], o_sem.at[2 * k + 1]))
    for cp in cps:
        cp.start()
    for cp in cps + stores:
        cp.wait()


def gw_call(first, last, segs, spots_of, cnt, misc, rows_in, w, land, out, est):
    n, m = len(segs), len(land)
    lands = tuple(a.shape[0] for a in land)
    width = sum(segs)
    ins = [cnt, misc, *rows_in, w, *land] + ([] if first else [out])
    in_specs = [SMEM, SMEM] + [ANY] * (len(ins) - 2)
    shapes = [jax.ShapeDtypeStruct((VL, D), F32)] + [jax.ShapeDtypeStruct((s, D), F32) for s in segs]
    out_specs = [ANY] * (n + 1)
    scratch = [pltpu.VMEM((2, CHUNK, D), BF16), pltpu.VMEM((width, D), BF16), pltpu.VMEM((width, D), F32), pltpu.VMEM((max(8, sum(lands)), D), F32),
               DMA((2,)), DMA((n,)), DMA((2 * n,)), DMA((max(m, 1),))]
    if first:
        shapes += [jax.ShapeDtypeStruct((ALL_ROWS, D), BF16), jax.ShapeDtypeStruct((8, 8, CHUNK), F32), jax.ShapeDtypeStruct((TBL,), jnp.int32)]
        out_specs += [ANY, VMEM, SMEM]
        scratch = [pltpu.VMEM((2, CHUNK, D), F32), pltpu.VMEM((2, CHUNK, LANE), F32), DMA((2,)), DMA((2,))] + scratch
    else:
        in_specs[2] = VMEM
    res = pl.pallas_call(
        functools.partial(gw_kernel, first, last, segs, lands, spots_of),
        in_specs=in_specs,
        out_specs=out_specs,
        out_shape=shapes,
        scratch_shapes=scratch,
        input_output_aliases={} if first else {len(ins) - 1: 0},
        compiler_params=params(63.5),
        cost_estimate=cost(est, 40e6),
    )(*ins)
    return res[0], res[1:1 + n], res[1 + n:]


def place_kernel(nsrc, rows, depth, spots_of, *refs):
    where = spots_of()
    srcs, out_ref, (buf, in_sem, out_sem) = refs[:nsrc], refs[nsrc + 1], refs[nsrc + 2:]
    jobs = []
    for k in range(nsrc):
        n = srcs[k].shape[0]
        for r in range(0, n, rows):
            jobs.append((k, r, min(rows, n - r)))

    def load(q):
        k, r, size = jobs[q]
        return pltpu.make_async_copy(srcs[k].at[pl.ds(r, size), :], buf.at[q % depth, pl.ds(0, size), :], in_sem.at[q % depth])

    def store(q):
        k, r, size = jobs[q]
        dst = out_ref.at[pl.ds(pl.multiple_of(where[k], 8) + r, size), :]
        return pltpu.make_async_copy(buf.at[q % depth, pl.ds(0, size), :], dst, out_sem.at[q % depth])

    lead = depth // 2
    for q in range(len(jobs) + lead):
        if q < len(jobs):
            if q >= depth:
                store(q - depth).wait()
            load(q).start()
        if q >= lead:
            load(q - lead).wait()
            store(q - lead).start()
    for q in range(max(0, len(jobs) - depth), len(jobs)):
        store(q).wait()


def place_call(spots_of, srcs, out):
    rows, depth, n = 160, 16, len(srcs)
    return pl.pallas_call(
        functools.partial(place_kernel, n, rows, depth, spots_of),
        in_specs=[ANY] * (n + 1),
        out_specs=ANY,
        out_shape=jax.ShapeDtypeStruct((VL, D), F32),
        scratch_shapes=[pltpu.VMEM((depth, rows, D), F32), DMA((depth,)), DMA((depth,))],
        input_output_aliases={n: 0},
        compiler_params=params(63.5),
        cost_estimate=cost(1e9, 80e6),
    )(*srcs, out)


def finish_kernel(du_ref, hid_ref, gamma_ref, gh_ref, gg_ref):
    x = hid_ref[...].astype(F32)
    r = lax.rsqrt(jnp.mean(x * x, axis=-1, keepdims=True) + EPS)
    n = x * r
    du = du_ref[...]
    v = du * gamma_ref[...].reshape(1, D)
    gh_ref[...] = (r * (v - n * jnp.mean(v * n, axis=-1, keepdims=True))).astype(BF16)

    @pl.when(pl.program_id(0) == 0)
    def _():
        gg_ref[...] = jnp.zeros_like(gg_ref)

    gg_ref[...] += jnp.sum(du * n, axis=0, keepdims=True)


def finish_call(du, hidden, gamma):
    rows = du.shape[0]
    block = 256
    return pl.pallas_call(
        finish_kernel,
        grid=(rows // block,),
        in_specs=[pl.BlockSpec((block, D), lambda i: (i, 0)), pl.BlockSpec((block, D), lambda i: (i, 0)), VMEM],
        out_specs=[pl.BlockSpec((block, D), lambda i: (i, 0)), pl.BlockSpec((1, D), lambda i: (0, 0))],
        out_shape=[jax.ShapeDtypeStruct((rows, D), BF16), jax.ShapeDtypeStruct((1, D), F32)],
        compiler_params=params(63.5),
        cost_estimate=cost(1e9, 13e6),
        name="finish",
    )(du, hidden, gamma)


MESH = pl.DeviceIdType.MESH
VB = 512
NFULL = VL // VB
TAIL = VL - NFULL * VB
ROWS = 1024
NSLOT = 3
NMSG = 80
POLL = (4, 6, 10, 12, 0, 2, 7, 14)


def own_kernel(hid_hbm, gamma_ref, w_hbm, lab_ref, mask_ref, u_out, du_out, sa_out, mine_out, cnt_out, misc_ref,
               z_ref, wbuf, du, ub_ref, m_ref, s_ref, l_ref, first_ref, st_buf, st_mine, lz_buf, lab_all, mask_all,
               ssem, rsem, s_send, s_recv, m_send, m_recv, l_send, l_recv, w_sem, c_sem):
    zi, yi, xi, ci = (lax.axis_index(n) for n in ("z", "y", "x", "c"))
    tp = zi * 4 + yi
    rank = xi * 2 + ci
    up = lambda i: lax.rem(i + 1, 4)
    dn = lambda i: lax.rem(i + 3, 4)
    op = lambda i: lax.rem(i + 2, 4)
    xp, xm, x2 = up(xi), dn(xi), op(xi)
    yp, ym, y2 = up(yi), dn(yi), op(yi)
    zp, zm, z2 = up(zi), dn(zi), op(zi)
    plane = [lax.rem(tp + k, 16) for k in range(1, 16)]
    line = [lax.rem(rank + k, 8) for k in range(1, 8)]
    pid = lambda q: {"z": q // 4, "y": lax.rem(q, 4)}
    lid = lambda q: {"x": q // 2, "c": lax.rem(q, 2)}

    def remote(src, dst, ssem_, rsem_, dev):
        return pltpu.make_async_remote_copy(src_ref=src, dst_ref=dst, send_sem=ssem_, recv_sem=rsem_, device_id=dev, device_id_type=MESH)

    al, lo, hi = pl.ds(0, 4), pl.ds(0, 32), pl.ds(32, 32)

    def regions(c):
        rm, rp, r2 = 2 * xm + c, 2 * xp + c, 2 * x2 + c
        return dict(
            a0=lambda z, y: u_out.at[rm, z, y, lo], b0=lambda z, y: u_out.at[r2, z, y, lo],
            a1=lambda z, y: u_out.at[rp, z, y, hi], b1=lambda z, y: u_out.at[r2, z, y, hi],
            a0r=lambda z: u_out.at[rm, z, al, lo], b0r=lambda z: u_out.at[r2, z, al, lo],
            a1c=lambda y: u_out.at[rp, al, y, hi], b1c=lambda y: u_out.at[r2, al, y, hi],
            xdm=u_out.at[rm, al, al, hi], xdp=u_out.at[rp, al, al, lo],
        )

    R, Q = regions(ci), regions(1 - ci)
    X_P, X_M = {"x": xp}, {"x": xm}
    Y_P, Y_M, Z_P, Z_M, PAL = {"y": yp}, {"y": ym}, {"z": zp}, {"z": zm}, {"c": 1 - ci}
    own = u_out.at[rank]
    msgs = {}

    def add(name, src, dev, arrives, dst=None):
        msgs[name] = (len(msgs), src, src if dst is None else dst, dev, arrives)

    add("P+", mine_out.at[lo], X_P, R["a0"](zi, yi), u_out.at[rank, zi, yi, lo])
    add("P-", mine_out.at[hi], X_M, R["a1"](zi, yi), u_out.at[rank, zi, yi, hi])
    add("F+", R["a0"](zi, yi), X_P, R["b0"](zi, yi))
    add("F-", R["a1"](zi, yi), X_M, R["b1"](zi, yi))
    add("XD+", u_out.at[rank, al, al, hi], X_P, R["xdm"])
    add("XD-", u_out.at[rank, al, al, lo], X_M, R["xdp"])
    ys, zs = dict(o=yi, m=ym, p=yp, t=y2), dict(o=zi, m=zm, p=zp, t=z2)
    for h, dp, dm in (("b0", Y_P, Y_M), ("b1", Z_P, Z_M)):
        f = R[h]
        nm, np_, n2 = ((zi, ym), (zi, yp), (zi, y2)) if h == "b0" else ((zm, yi), (zp, yi), (z2, yi))
        add(h + "+", f(zi, yi), dp, f(*nm))
        add(h + "-", f(zi, yi), dm, f(*np_))
        add(h + "f", f(*np_), dm, f(*n2))
    for h, dp, dm in (("a0", Y_P, Y_M), ("a1", Z_P, Z_M)):
        f = R[h]
        nm, np_, n2 = ((zi, ym), (zi, yp), (zi, y2)) if h == "a0" else ((zm, yi), (zp, yi), (z2, yi))
        add(h + "+", f(zi, yi), dp, f(*nm))
        add(h + "-", f(zi, yi), dm, f(*np_))
        add(h + "f", f(*nm), dp, f(*n2))
    for k in "ompt":
        for h in "AB":
            f, e = R[h.lower() + "0"], R[h.lower() + "1"]
            add(h + "0+" + k, f(zi, ys[k]), Z_P, f(zm, ys[k]))
            add(h + "0-" + k, f(zi, ys[k]), Z_M, f(zp, ys[k]))
            add(h + "1+" + k, e(zs[k], yi), Y_P, e(zs[k], ym))
            add(h + "1-" + k, e(zs[k], yi), Y_M, e(zs[k], yp))
    add("A0f", R["a0r"](zm), Z_P, R["a0r"](z2))
    add("A1f", R["a1c"](ym), Y_P, R["a1c"](y2))
    add("B0f", R["b0r"](zp), Z_M, R["b0r"](z2))
    add("B1f", R["b1c"](yp), Y_M, R["b1c"](y2))
    add("Down", own, PAL, u_out.at[2 * xi + 1 - ci])
    add("Dx+", R["xdm"], PAL, Q["xdm"])
    add("Dx-", R["xdp"], PAL, Q["xdp"])
    for k in "ompt":
        for h, i in (("a0r", zs[k]), ("b0r", zs[k]), ("a1c", ys[k]), ("b1c", ys[k])):
            add("D" + h + k, R[h](i), PAL, Q[h](i))
    assert len(msgs) <= NMSG
    on_chip = [n for n in msgs if n[0] == "D"]

    def send(*names):
        for n in names:
            k, src, dst, dev, _ = msgs[n]
            remote(src, dst, ssem.at[k], rsem.at[k], dev).start()

    def got(*names):
        for n in names:
            k, _, _, dev, reg = msgs[n]
            remote(reg, reg, ssem.at[k], rsem.at[k], dev).wait_recv()

    def w_copies(j, slot, size=VB):
        part = size // 4 // 8 * 8
        cuts = [0, part, 2 * part, 3 * part, size]
        return [pltpu.make_async_copy(w_hbm.at[pl.ds(pl.multiple_of(j * VB + a, 8), b - a), :], wbuf.at[slot, pl.ds(a, b - a)], w_sem.at[slot])
                for a, b in zip(cuts[:-1], cuts[1:])]

    def w_start(j, slot, size=VB):
        for cp in w_copies(j, slot, size):
            cp.start()

    def w_wait(slot, size=VB):
        pltpu.make_async_copy(w_hbm.at[pl.ds(0, size), :], wbuf.at[slot, pl.ds(0, size)], w_sem.at[slot]).wait()

    slice_in = pltpu.make_async_copy(hid_hbm.at[pl.ds(pl.multiple_of(tp * SLICE, SLICE), SLICE)], ub_ref.at[pl.ds(0, SLICE)], c_sem.at[0])
    slice_in.start()
    bar = pltpu.get_barrier_semaphore()
    for q in plane:
        pl.semaphore_signal(bar, inc=1, device_id=pid(q), device_id_type=MESH)
    for q in line:
        pl.semaphore_signal(bar, inc=1, device_id=lid(q), device_id_type=MESH)

    def unit(v):
        x = v.astype(F32)
        r = lax.rsqrt(jnp.mean(x * x, axis=-1, keepdims=True) + EPS)
        return (x * r * gamma_ref[...].reshape(1, D)).astype(BF16)

    slice_in.wait()
    first_ref[...] = unit(ub_ref[0:SLICE]).astype(F32)
    slice_out = pltpu.make_async_copy(first_ref, mine_out, c_sem.at[0])
    slice_out.start()
    rows_in = [pltpu.make_async_copy(hid_hbm.at[pl.ds(256 * t, 256)], ub_ref.at[pl.ds(256 * t, 256)], w_sem.at[t % 2]) for t in range(4)]
    for t in range(2):
        rows_in[t].start()
    pl.semaphore_wait(bar, 22)
    line_msgs = []
    for k, q in enumerate(line):
        for i, (ref, dst) in enumerate(((lab_ref, lab_all), (mask_ref, mask_all))):
            cp = remote(ref, dst.at[rank], m_send.at[i, k], m_recv.at[i, rank], lid(q))
            cp.start()
            line_msgs.append(cp)
    lab_all[rank] = lab_ref[...]
    mask_all[rank] = mask_ref[...]
    slice_out.wait()
    send("P+", "P-")
    local = []
    for t in range(4):
        rows_in[t].wait()
        if t < 2:
            rows_in[t + 2].start()
        rs = pl.ds(256 * t, 256)
        u = unit(ub_ref[rs, :])
        ub_ref[rs, :] = u
        du[rs, :] = u.astype(F32)
        for k in range(4):
            cp = pltpu.make_async_copy(du.at[pl.ds(256 * t + SLICE * k, SLICE)], u_out.at[rank, t, k], c_sem.at[1])
            cp.start()
            local.append(cp)
    for j in range(NSLOT - 1):
        w_start(j, j)
    for cp in local:
        cp.wait()
    spread = lambda h, ks: send(*[h + i + d + k for k in ks for i in "01" for d in "+-"])
    came = lambda h, d: got(*[h + i + d + k for k in "ompt" for i in "01"])
    got("P+", "P-")
    send("F+", "F-", "a0+", "a0-", "a1+", "a1-", "XD+", "XD-", "Down")
    spread("A", "o")
    m_ref[...] = jnp.full_like(m_ref, -BIG)
    s_ref[...] = jnp.zeros_like(s_ref)
    l_ref[...] = jnp.zeros_like(l_ref)

    as_row = lambda v: jnp.concatenate([v[i:i + 1, :] for i in range(8)], axis=1)
    as_tile = lambda v: jnp.concatenate([v[:, LANE * i:LANE * i + LANE] for i in range(8)], axis=0)
    seq_row = lambda v: jnp.concatenate([v[0:1, :], v[1:2, :]], axis=1)
    lab = seq_row((lab_ref[...] - tp * VL).astype(F32))
    on = seq_row(mask_ref[...]) > 0

    def stats(j, slot, size):
        z = lax.dot_general(wbuf[slot, :size], ub_ref[...], (((1,), (1,)), ((), ())), preferred_element_type=F32)
        z_ref[pl.ds(pl.multiple_of(j * VB, 8), size), :] = z
        zz = z.reshape(size // 8, 8, ROWS)
        ids = lax.broadcasted_iota(jnp.int32, (size, ROWS), 0).astype(F32)
        rel = lab - (j * VB) * 1.0
        m_old = m_ref[...]
        m_new = jnp.maximum(m_old, jnp.max(zz, axis=0))
        s_ref[...] = s_ref[...] * jnp.exp(m_old - m_new) + jnp.sum(jnp.exp(zz - m_new[None]), axis=0)
        l_ref[...] += jnp.sum(jnp.where(ids == rel, z, 0.0).reshape(size // 8, 8, ROWS), axis=0)
        m_ref[...] = m_new

    def at(j, k, fn):
        @pl.when(j == k)
        def _():
            fn()

    def stream(j):
        slot = lax.rem(j, NSLOT)
        w_wait(slot)
        ahead = j + NSLOT - 1
        to = lax.rem(ahead, NSLOT)

        @pl.when(ahead < NFULL)
        def _():
            w_start(ahead, to)

        @pl.when(ahead == NFULL)
        def _():
            w_start(NFULL, to, TAIL)

        return slot

    def near_a():
        got("a0+", "a1+")
        send("a0f", "a1f")
        spread("A", "m")
        got("a0-", "a1-")
        spread("A", "p")

    def first_b():
        got("F+", "F-")
        send("b0+", "b0-", "b1+", "b1-")
        spread("B", "o")

    def far_a():
        got("a0f", "a1f")
        spread("A", "t")
        send("Da0ro", "Da1co")

    def near_b():
        got("b0-", "b1-")
        send("b0f", "b1f")

    def stats_step(j, _):
        slot = stream(j)
        stats(j, slot, VB)
        at(j, POLL[0], near_a)
        at(j, POLL[1], first_b)
        at(j, POLL[2], far_a)
        at(j, POLL[3], near_b)
        return 0

    lax.fori_loop(0, NFULL, stats_step, 0)
    w_wait(NFULL % NSLOT, TAIL)
    stats(NFULL, NFULL % NSLOT, TAIL)
    for j in range(NSLOT - 1):
        w_start(j, j)

    m8 = m_ref[...]
    top = jnp.max(m8, axis=0, keepdims=True)
    tot = jnp.sum(s_ref[...] * jnp.exp(m8 - top), axis=0, keepdims=True)
    hit = jnp.sum(l_ref[...], axis=0, keepdims=True)
    for k, v in enumerate((top, tot, hit)):
        st_mine[k] = as_tile(v)
        st_buf[tp, k] = as_tile(v)
    plane_msgs = []
    for k, q in enumerate(plane):
        cp = remote(st_mine, st_buf.at[tp], s_send.at[k], s_recv.at[tp], pid(q))
        cp.start()
        plane_msgs.append(cp)
    got("b0+", "b1+")
    spread("B", "pm")
    got("b0f", "b1f")
    spread("B", "t")
    send("Db0ro", "Db1co")
    for k, q in enumerate(line):
        for i, (ref, dst) in enumerate(((lab_ref, lab_all), (mask_ref, mask_all))):
            remote(ref, dst.at[q], m_send.at[i, k], m_recv.at[i, q], lid(q)).wait_recv()
    count = jnp.zeros((1, 1), F32)
    for r in range(8):
        for s in range(2):
            c = jnp.sum(mask_all[r, s:s + 1, :].astype(F32), axis=1, keepdims=True)
            cnt_out[2 * r + s] = jnp.sum(c).astype(jnp.int32)
            count += c
    log_n = jnp.log(count)
    winv = 1.0 / count
    for k, q in enumerate(plane):
        remote(st_mine, st_buf.at[q], s_send.at[k], s_recv.at[q], pid(q)).wait_recv()
    top = st_buf[0, 0]
    for q in range(1, 16):
        top = jnp.maximum(top, st_buf[q, 0])
    total = jnp.zeros_like(top)
    label = jnp.zeros_like(top)
    for q in range(16):
        total += st_buf[q, 1] * jnp.exp(st_buf[q, 0] - top)
        label += st_buf[q, 2]
    lse = top + jnp.log(total)
    lz_buf[rank, 0] = lse
    lz_buf[rank, 1] = label
    shift = jnp.where(on, as_row(lse) + log_n, BIG)
    lab_on = jnp.where(on, lab, -BIG)
    for k, q in enumerate(line):
        cp = remote(lz_buf.at[rank], lz_buf.at[rank], l_send.at[k], l_recv.at[rank], lid(q))
        cp.start()
        line_msgs.append(cp)

    du[...] = jnp.zeros_like(du)

    def grad(j, slot, size):
        z = z_ref[pl.ds(pl.multiple_of(j * VB, 8), size), :]
        ids = lax.broadcasted_iota(jnp.int32, (size, ROWS), 0).astype(F32)
        rel = lab_on - (j * VB) * 1.0
        g = (jnp.exp(z - shift) - jnp.where(ids == rel, winv, 0.0)).astype(BF16)
        du[...] += lax.dot_general(g, wbuf[slot, :size], (((0,), (0,)), ((), ())), preferred_element_type=F32)

    def arrive_a():
        came("A", "+")
        send("A0f", "A1f", "Da0rm", "Da1cm")

    def arrive_a2():
        came("A", "-")
        send("Da0rp", "Da1cp")

    def arrive_b():
        came("B", "-")
        send("B0f", "B1f", "Db0rp", "Db1cp")
        came("B", "+")
        send("Db0rm", "Db1cm")

    def arrive_x():
        got("XD+")
        send("Dx+")
        got("XD-")
        send("Dx-")

    def grad_step(j, _):
        slot = stream(j)
        grad(j, slot, VB)
        at(j, POLL[4], arrive_a)
        at(j, POLL[5], arrive_a2)
        at(j, POLL[6], arrive_b)
        at(j, POLL[7], arrive_x)
        return 0

    lax.fori_loop(0, NFULL, grad_step, 0)
    w_wait(NFULL % NSLOT, TAIL)
    grad(NFULL, NFULL % NSLOT, TAIL)
    outs = [pltpu.make_async_copy(du, du_out, c_sem.at[0])]
    outs[0].start()

    for k, q in enumerate(line):
        remote(lz_buf.at[q], lz_buf.at[q], l_send.at[k], l_recv.at[q], lid(q)).wait_recv()
    loss = jnp.zeros((1, 1), F32)
    left = lax.broadcasted_iota(jnp.int32, (LANE, LANE), 0) < SLICE
    for r in range(8):
        for s in range(2):
            for q in range(4):
                cols = slice(LANE * q, LANE * q + LANE)
                live = mask_all[r, s:s + 1, cols] > 0
                ids = jnp.where(live, (lab_all[r, s:s + 1, cols] - tp * VL).astype(F32), -BIG)
                i = 4 * s + q
                lse = lz_buf[r, 0, i:i + 1, :]
                loss += jnp.sum(jnp.where(live, (lse - lz_buf[r, 1, i:i + 1, :]) / count, 0.0), axis=1, keepdims=True)
                sh = jnp.where(live, lse + log_n, BIG)
                both = jnp.where(left, jnp.broadcast_to(sh, (LANE, LANE)), jnp.broadcast_to(ids, (LANE, LANE)))
                z_ref[pl.ds(r * 1024 + i * LANE, LANE), 0:LANE] = jnp.transpose(both)
    z_ref[pl.ds(ALL_ROWS, GROUP), 0:LANE] = jnp.where(lax.broadcasted_iota(jnp.int32, (GROUP, LANE), 1) < SLICE, BIG, -BIG)
    outs.append(pltpu.make_async_copy(z_ref.at[pl.ds(0, ALL_ROWS + GROUP), pl.ds(0, LANE)], sa_out, c_sem.at[1]))
    outs[1].start()
    sub = lax.broadcasted_iota(jnp.int32, (8, LANE), 0)
    misc_ref[...] = jnp.where(sub == 0, jnp.broadcast_to(loss, (8, LANE)), jnp.broadcast_to(winv, (8, LANE)))
    got("A0f", "A1f")
    send("Da0rt", "Da1ct")
    got("B0f", "B1f")
    send("Db0rt", "Db1ct")
    got(*on_chip)
    for cp in line_msgs + plane_msgs:
        cp.wait_send()
    for (k, src, dst, dev, _) in msgs.values():
        remote(src, dst, ssem.at[k], rsem.at[k], dev).wait_send()
    for cp in outs:
        cp.wait()


def own_call(hidden, gamma, wt, labels, mask):
    return pl.pallas_call(
        own_kernel,
        in_specs=[ANY, VMEM, ANY, VMEM, VMEM],
        out_specs=[ANY, ANY, ANY, ANY, SMEM, VMEM],
        out_shape=[
            jax.ShapeDtypeStruct((8, 4, 4, SLICE, D), F32),
            jax.ShapeDtypeStruct((ROWS, D), F32),
            jax.ShapeDtypeStruct((ALL_ROWS + GROUP, LANE), F32),
            jax.ShapeDtypeStruct((SLICE, D), F32),
            jax.ShapeDtypeStruct((16,), jnp.int32),
            jax.ShapeDtypeStruct((8, LANE), F32),
        ],
        scratch_shapes=[
            pltpu.VMEM((VL, ROWS), F32), pltpu.VMEM((NSLOT, VB, D), BF16), pltpu.VMEM((ROWS, D), F32), pltpu.VMEM((ROWS, D), BF16),
            pltpu.VMEM((8, ROWS), F32), pltpu.VMEM((8, ROWS), F32), pltpu.VMEM((8, ROWS), F32),
            pltpu.VMEM((SLICE, D), F32), pltpu.VMEM((16, 3, 8, LANE), F32), pltpu.VMEM((3, 8, LANE), F32), pltpu.VMEM((8, 2, 8, LANE), F32),
            pltpu.VMEM((8, 2, 512), jnp.int32), pltpu.VMEM((8, 2, 512), jnp.int32),
            DMA((NMSG,)), DMA((NMSG,)), DMA((15,)), DMA((16,)), DMA((2, 7)), DMA((2, 8)), DMA((7,)), DMA((8,)), DMA((NSLOT,)), DMA((2,)),
        ],
        compiler_params=params(63.5, collective_id=0, has_side_effects=True),
        cost_estimate=cost(1e9, 200e6),
        name="own_rank",
    )(hidden, gamma, wt, labels, mask)


SEG0, SEG1 = 320, 512
S_ROWS = 2 * (SEG0 + SEG1)
C_ROWS = (840, 584)
EST = 1e9


HALF_ROWS = 4752
C_LAST = VL - C_ROWS[1]


def spots(kind, k):
    xi, ci = lax.axis_index("x"), lax.axis_index("c")
    core = ci if kind in ("mine", "gain", "c") else 1 - ci
    base = core * HALF_ROWS
    if kind[0] == "c":
        start = base + 2 * S_ROWS + (0, C_ROWS[0])[k]
        return jnp.minimum(start, C_LAST) if k else start
    flip = lax.rem(xi, 2) if kind in ("gain", "gain2") else 1 - lax.rem(xi, 2)
    return base + flip * S_ROWS + (0, SEG0 + SEG1, SEG0, 2 * SEG0 + SEG1)[k]


def at_spots(*names):
    return lambda: [spots(n, k) for n, k in names]


def local_step(hidden, gamma, w, labels, mask):
    num_seqs, seqlen, _ = hidden.shape
    tokens = num_seqs * seqlen
    wt = w.T
    hidden = hidden.reshape(tokens, D)
    u_all, du, sa, _, cnt, misc = own_call(hidden, gamma, wt, labels, mask)
    u_all = u_all.reshape(ALL_ROWS, D)
    loss = misc[0, 0]
    mesh_size = {"x": 4, "c": 2}

    def hop(a, axis="c", step=1):
        k = mesh_size[axis]
        return lax.ppermute(a, axis, [(i, (i + step) % k) for i in range(k)])

    def gw(name, segs, mine, lands, where, last=False):
        spots_of = lambda: (at_spots(*mine)(), at_spots(*where)())
        if name == "gw0":
            return gw_call(True, False, segs, spots_of, cnt, misc, (u_all, sa), wt, [], None, EST)
        return gw_call(False, last, segs, spots_of, tbl, misc, (side, uc), wt, lands, out, EST)

    pair = lambda n, k: [(n, k), (n, k + 1)]
    out, (l0, r0), (uc, side, tbl) = gw("gw0", (SEG0, SEG0), pair("mine", 0), [], [])
    xl0, xr0 = hop(l0, "x", 3), hop(r0, "x", 1)
    dl0, dr0 = hop(l0), hop(r0)
    out, (l1, r1), _ = gw("gw1", (SEG1, SEG1), pair("mine", 2), [l0, r0], pair("mine", 0))
    xl1, xr1 = hop(l1, "x", 3), hop(r1, "x", 1)
    dl1, dr1 = hop(l1), hop(r1)
    out, (c0,), _ = gw("gw2", C_ROWS[:1], [("c", 0)], [l1, r1, dl0, dr0], pair("mine", 2) + pair("theirs", 0))
    dc0 = hop(c0)
    hl0, hr0 = hop(xl0), hop(xr0)
    out, (c1,), _ = gw("gw3", C_ROWS[1:], [("c", 1)], [c0, dl1, dr1, xl0, xr0], [("c", 0)] + pair("theirs", 2) + pair("gain", 0), True)
    dc1 = hop(c1)
    hl1, hr1 = hop(xl1), hop(xr1)
    out = place_call(at_spots(("c2", 0), *pair("gain2", 0), *pair("gain", 2)), [dc0, hl0, hr0, xl1, xr1], out)
    grad_w = place_call(at_spots(*pair("gain2", 2), ("c2", 1)), [hl1, hr1, dc1], out).T

    du = lax.psum(du, ("z", "y"))
    grad_hidden, gg = finish_call(du, hidden, gamma)
    gg = gg + hop(gg, "x", 2)
    gg = gg + hop(gg, "x", 1)
    grad_gamma = (gg + hop(gg)).reshape(D)
    return loss, grad_hidden.reshape(num_seqs, seqlen, D), grad_w, grad_gamma


def solution(mesh):
    fine = Mesh(mesh.devices.reshape(4, 4, 4, 2), ("z", "y", "x", "c"))

    return jax.shard_map(
        local_step,
        mesh=fine,
        in_specs=(P(("x", "c"), None, None), P(), P(None, ("z", "y")), P(("x", "c"), None), P(("x", "c"), None)),
        out_specs=(P(), P(("x", "c"), None, None), P(None, ("z", "y")), P()),
        check_vma=False,
    )
```
